32 devices in a mesh: dp: 8 (over z, y), tensor: 4 (over x, core).
Axes of the slice: x: 2, y: 2, z: 4, core: 2. Of those that a mesh axis runs over, the one named last changes fastest.
Arguments:
- attention_output: bfloat16 [4096, 8192], P('dp', 'tensor'), may hold values from -6 to 6
- frozen_weight: bfloat16 [8192, 8192], P('tensor'), may hold values from -0.0625 to 0.0625
- output_gradient: bfloat16 [4096, 8192], P('dp', 'tensor'), may hold values from -6 to 6
- tenant_token_count: int32 [8, 32], P('dp'), may hold values from 1 to 256, 512 in all within a row
- tenant_storage_slot: int32 [32], replicated, may hold values from 0 to 31, each once
- adapter_down_weight: float32 [32, 8192, 16], P('dp', 'tensor'), may hold values from -0.0625 to 0.0625
- adapter_up_weight: float32 [32, 16, 8192], P('dp', None, 'tensor'), may hold values from -1.5 to 1.5
- down_first_moment: float32 [32, 8192, 16], P('dp', 'tensor'), may hold values from -60 to 60
- down_second_moment: float32 [32, 8192, 16], P('dp', 'tensor'), may hold values from 1 to 10000
- up_first_moment: float32 [32, 16, 8192], P('dp', None, 'tensor'), may hold values from -60 to 60
- up_second_moment: float32 [32, 16, 8192], P('dp', None, 'tensor'), may hold values from 1 to 10000
Outputs:
- proj_out: bfloat16 [4096, 8192], P('dp', 'tensor')
- input_grad: bfloat16 [4096, 8192], P('dp', 'tensor')
- updated_down_weight: float32 [32, 8192, 16], P('dp', 'tensor')
- updated_up_weight: float32 [32, 16, 8192], P('dp', None, 'tensor')
- updated_down_first_moment: float32 [32, 8192, 16], P('dp', 'tensor')
- updated_down_second_moment: float32 [32, 8192, 16], P('dp', 'tensor')
- updated_up_first_moment: float32 [32, 16, 8192], P('dp', None, 'tensor')
- updated_up_second_moment: float32 [32, 16, 8192], P('dp', None, 'tensor')
The draws below stay inside these ranges and needn't reach their ends.
Inputs may be any that keep to these rules, and one draw needn't show every extreme that they name: `tenant_token_count`: each row sums to 512; every tenant has at least one token in every row; tokens of one dp index are sorted by tenant. `tenant_storage_slot`: a permutation of the slots.
All inputs are finite; a program needn't handle non-finite values.
Results may differ from the reference program's by a relative error of at most 0.02.
Values may be sent and summed in bfloat16 or wider, within the bound.
A program may use at most 128 MiB of HBM per device.

```python
import math
import jax
import jax.numpy as jnp
import numpy as np
from jax import lax

MODEL_WIDTH = 8192
ADAPTER_RANK = 16
TOK_DEV = 512
TENANT_TOTAL = 32
TOKENS = 4096
N_DP = 8
N_TENSOR = 4


def block_scale(stream_key, dims, cuts, low, top_value):
    factor_of, own = 1.0, jax.random.fold_in(stream_key, 6)
    for position, parts in cuts:
        steps = jnp.exp(jax.random.uniform(jax.random.fold_in(own, position), (parts,), jnp.float32, low / len(cuts), top_value / len(cuts)))
        factor_of = factor_of * jnp.repeat(steps, dims[position] // parts).reshape([-1 if axis == position else 1 for axis in range(len(dims))])
    return factor_of


def length_profile(number_of, total, limit, slope):
    loads = [(1 << 20) // math.isqrt(standing ** slope) + 1 for standing in range(2, number_of + 1)]
    rest, counts = total - limit - (number_of - 1), [1] * (number_of - 1)
    while rest > 0:
        candidates = [i for i in range(number_of - 1) if counts[i] < limit]
        mass, budget = sum([loads[i] for i in candidates]), rest
        for i in candidates:
            more = min(limit - counts[i], max(1, budget * loads[i] // mass), rest)
            counts[i] = counts[i] + more
            rest = rest - more
    return np.array([limit] + counts)


def ragged(rng, number_of, total, bound, lean):
    if number_of == 2:
        one = jax.random.randint(rng, (), max(1, total - bound), min(bound, total - 1) + 1)
        return jnp.stack([one, total - one])
    tallies = jnp.asarray(length_profile(number_of, total, bound, lean), jnp.int32)
    pairs = (number_of - 1) // 2
    giver, taker = tallies[1:1 + 2 * pairs:2], tallies[2:2 + 2 * pairs:2]
    slack = jnp.minimum(giver - 1, bound - taker)
    passed = jax.random.randint(jax.random.fold_in(rng, 1), (pairs,), 0, 1 << 20) % (slack + 1)
    tallies = tallies.at[1:1 + 2 * pairs:2].set(giver - passed).at[2:2 + 2 * pairs:2].set(taker + passed)
    return tallies[jax.random.permutation(jax.random.fold_in(rng, 2), number_of)]


def bell_draw(own_key, shape, scale, most, split=(), kind=jnp.bfloat16):
    gain = block_scale(own_key, shape, split, -0.22, 0.18) if split else 1.0
    array = jax.random.normal(own_key, shape, jnp.float32) * scale * gain
    return jnp.minimum(jnp.maximum(array, -most), most).astype(kind)


def setup_inputs(seed: int = 0) -> dict:
    keys = jax.random.split(jax.random.key(seed), 12)
    attention_output = bell_draw(keys[0], (TOKENS, MODEL_WIDTH), 1.0, 6.0, ((0, 8), (1, 4)))
    frozen_weight = bell_draw(keys[1], (MODEL_WIDTH, MODEL_WIDTH), MODEL_WIDTH ** -0.5, 0.0625, ((0, 4),))
    output_gradient = bell_draw(keys[2], (TOKENS, MODEL_WIDTH), 1.0, 6.0, ((0, 8), (1, 4)))
    tenant_token_count = jax.vmap(lambda own: ragged(own, TENANT_TOTAL, TOK_DEV, TOK_DEV // 2, 2))(jax.random.split(keys[3], N_DP)).reshape((N_DP, TENANT_TOTAL)).astype(jnp.int32)
    tenant_storage_slot = jax.random.permutation(keys[4], TENANT_TOTAL).astype(jnp.int32)
    adapter_down_weight = bell_draw(keys[5], (TENANT_TOTAL, MODEL_WIDTH, ADAPTER_RANK), MODEL_WIDTH ** -0.5, 0.0625, ((0, 8), (1, 4)), jnp.float32)
    adapter_up_weight = bell_draw(keys[6], (TENANT_TOTAL, ADAPTER_RANK, MODEL_WIDTH), ADAPTER_RANK ** -0.5, 1.5, ((0, 8), (2, 4)), jnp.float32)
    down_first_moment = bell_draw(keys[7], (TENANT_TOTAL, MODEL_WIDTH, ADAPTER_RANK), 10.0, 60.0, ((0, 8), (1, 4)), jnp.float32)
    down_second_moment = jnp.clip(jnp.exp(math.log(10000.0) - 9.2103404 * jax.random.uniform(keys[8], (TENANT_TOTAL, MODEL_WIDTH, ADAPTER_RANK), jnp.float32) ** block_scale(keys[8], (TENANT_TOTAL, MODEL_WIDTH, ADAPTER_RANK), ((0, 8), (1, 4)), -0.2, 0.2)), 1.0, 10000.0)
    up_first_moment = bell_draw(keys[9], (TENANT_TOTAL, ADAPTER_RANK, MODEL_WIDTH), 10.0, 60.0, ((0, 8), (2, 4)), jnp.float32)
    up_second_moment = jnp.clip(jnp.exp(math.log(10000.0) - 9.2103404 * jax.random.uniform(keys[10], (TENANT_TOTAL, ADAPTER_RANK, MODEL_WIDTH), jnp.float32) ** block_scale(keys[10], (TENANT_TOTAL, ADAPTER_RANK, MODEL_WIDTH), ((0, 8), (2, 4)), -0.2, 0.2)), 1.0, 10000.0)
    return {"attention_output": attention_output, "frozen_weight": frozen_weight, "output_gradient": output_gradient, "tenant_token_count": tenant_token_count, "tenant_storage_slot": tenant_storage_slot, "adapter_down_weight": adapter_down_weight, "adapter_up_weight": adapter_up_weight, "down_first_moment": down_first_moment, "down_second_moment": down_second_moment, "up_first_moment": up_first_moment, "up_second_moment": up_second_moment}


def adam_update(param, first, second, grad):
    first = 0.9 * first + 0.1 * grad
    second = 0.999 * second + 0.001 * grad * grad
    corr_one = 1.0 - 0.9 ** 10
    corr_two = 1.0 - 0.999 ** 10
    step_size = first / corr_one / (jnp.sqrt(second / corr_two) + 1e-08)
    return (param - 0.01 * (step_size + 0.1 * param), first, second)

def reference(attention_output, frozen_weight, output_gradient, tenant_token_count, tenant_storage_slot, adapter_down_weight, adapter_up_weight, down_first_moment, down_second_moment, up_first_moment, up_second_moment):
    positions = jnp.arange(TOK_DEV, dtype=jnp.int32)
    ends = jnp.cumsum(tenant_token_count, axis=1)
    tenant = lax.optimization_barrier(jnp.sum((ends[:, None, :] <= positions[None, :, None]).astype(jnp.int32), axis=-1)).reshape(-1)
    slot = tenant_storage_slot[tenant]
    onehot = (slot[:, None] == jnp.arange(TENANT_TOTAL, dtype=jnp.int32)[None, :]).astype(jnp.float32)
    down_half_precision = adapter_down_weight.astype(jnp.bfloat16)
    up_half_precision = adapter_up_weight.astype(jnp.bfloat16)
    down_flat = jnp.transpose(down_half_precision, (1, 0, 2)).reshape(MODEL_WIDTH, TENANT_TOTAL * ADAPTER_RANK)
    up_flat = up_half_precision.reshape(TENANT_TOTAL * ADAPTER_RANK, MODEL_WIDTH)
    low_all = jnp.dot(attention_output, down_flat, preferred_element_type=jnp.float32).reshape(-1, TENANT_TOTAL, ADAPTER_RANK)
    low = lax.optimization_barrier(jnp.sum(low_all * onehot[:, :, None], axis=1))
    low_wide = (onehot[:, :, None] * low[:, None, :]).reshape(-1, TENANT_TOTAL * ADAPTER_RANK).astype(jnp.bfloat16)
    width = MODEL_WIDTH // N_TENSOR

    def add_block(total, index):
        cols = lax.dynamic_slice_in_dim(attention_output, index * width, width, 1)
        rows = lax.dynamic_slice_in_dim(frozen_weight, index * width, width, 0)
        part = lax.optimization_barrier(jnp.dot(cols, rows, preferred_element_type=jnp.float32).astype(jnp.bfloat16))
        return (total + part.astype(jnp.float32), None)
    base, _ = lax.scan(add_block, jnp.zeros((TOKENS, MODEL_WIDTH), jnp.float32), jnp.arange(N_TENSOR, dtype=jnp.int32))
    proj_out = (base + 2.0 * jnp.dot(low_wide, up_flat, preferred_element_type=jnp.float32)).astype(jnp.bfloat16)
    back_all = lax.dot_general(output_gradient, up_flat, (((1,), (1,)), ((), ())), preferred_element_type=jnp.float32).reshape(-1, TENANT_TOTAL, ADAPTER_RANK)
    back = lax.optimization_barrier(jnp.sum(back_all * onehot[:, :, None], axis=1))
    back_wide = (onehot[:, :, None] * back[:, None, :]).reshape(-1, TENANT_TOTAL * ADAPTER_RANK).astype(jnp.bfloat16)
    grad_base = lax.dot_general(output_gradient, frozen_weight, (((1,), (1,)), ((), ())), preferred_element_type=jnp.float32)
    grad_low = lax.dot_general(back_wide, down_flat, (((1,), (1,)), ((), ())), preferred_element_type=jnp.float32)
    input_grad = (grad_base + 2.0 * grad_low).astype(jnp.bfloat16)
    down_gradient = 2.0 * lax.dot_general(attention_output, back_wide, (((0,), (0,)), ((), ())), preferred_element_type=jnp.float32)
    down_gradient = jnp.transpose(down_gradient.reshape(MODEL_WIDTH, TENANT_TOTAL, ADAPTER_RANK), (1, 0, 2))
    up_gradient = 2.0 * lax.dot_general(low_wide, output_gradient, (((0,), (0,)), ((), ())), preferred_element_type=jnp.float32)
    up_gradient = up_gradient.reshape(TENANT_TOTAL, ADAPTER_RANK, MODEL_WIDTH)
    updated_down_weight, updated_down_first_moment, updated_down_second_moment = adam_update(adapter_down_weight, down_first_moment, down_second_moment, down_gradient)
    updated_up_weight, updated_up_first_moment, updated_up_second_moment = adam_update(adapter_up_weight, up_first_moment, up_second_moment, up_gradient)
    return (proj_out, input_grad, updated_down_weight, updated_up_weight, updated_down_first_moment, updated_down_second_moment, updated_up_first_moment, updated_up_second_moment)
```

```python
import functools

import jax
import jax.numpy as jnp
from jax import lax
from jax.sharding import PartitionSpec as P


def adam_update(param, first, second, grad):
    first = 0.9 * first + 0.1 * grad
    second = 0.999 * second + 0.001 * grad * grad
    corr_one = 1.0 - 0.9**10
    corr_two = 1.0 - 0.999**10
    step_size = first / corr_one / (jnp.sqrt(second / corr_two) + 1e-08)
    return (param - 0.01 * (step_size + 0.1 * param), first, second)


def pair_and_rest(size):
    pair = 2 if size % 2 == 0 else 1
    return pair, size // pair


def flip(value, axis, size):
    return lax.ppermute(value, axis, [(i, i ^ 1) for i in range(size)])


def shift(value, axis, size, hops):
    pair, rest = pair_and_rest(size)
    hops = hops % rest
    return lax.ppermute(
        value,
        axis,
        [(r * pair + c, ((r + hops) % rest) * pair + c) for r in range(rest) for c in range(pair)],
    )


def sum_over(value, axis, size):
    pair, rest = pair_and_rest(size)
    if pair == 2:
        value = value + flip(value, axis, size)
    return sum((shift(value, axis, size, k) for k in range(1, rest)), value)


def local(
    n_dp,
    n_tensor,
    attention_output,
    frozen_weight,
    output_gradient,
    tenant_token_count,
    tenant_storage_slot,
    adapter_down_weight,
    adapter_up_weight,
    down_first_moment,
    down_second_moment,
    up_first_moment,
    up_second_moment,
):
    f32, bf16 = jnp.float32, jnp.bfloat16
    tok_rows, width = attention_output.shape
    tenants = tenant_storage_slot.shape[0]
    owned, _, rank = adapter_down_weight.shape
    wide = tenants * rank
    dp_pair, dp_rest = pair_and_rest(n_dp)
    t_pair, t_rest = pair_and_rest(n_tensor)
    dp_row, dp_col = lax.axis_index("dp") // dp_pair, lax.axis_index("dp") % dp_pair
    t_row, t_col = lax.axis_index("tensor") // t_pair, lax.axis_index("tensor") % t_pair

    blocks = []
    for k in range(t_rest):
        block = shift(output_gradient, "tensor", n_tensor, k) if k else output_gradient
        row = (t_row - k) % t_rest
        blocks.append((row * t_pair + t_col, block))
        if t_pair == 2:
            blocks.append((row * t_pair + 1 - t_col, flip(block, "tensor", n_tensor)))

    own_down = jnp.transpose(adapter_down_weight.astype(bf16), (0, 2, 1)).reshape(-1, width)
    own_up = adapter_up_weight.astype(bf16).reshape(-1, width)
    down_blocks, up_blocks, owners = [], [], []
    for k in range(dp_rest):
        down_k = shift(own_down, "dp", n_dp, k) if k else own_down
        up_k = shift(own_up, "dp", n_dp, k) if k else own_up
        row = (dp_row - k) % dp_rest
        down_blocks.append(down_k)
        up_blocks.append(up_k)
        owners.append(row * dp_pair + dp_col)
        if dp_pair == 2:
            down_blocks.append(flip(down_k, "dp", n_dp))
            up_blocks.append(flip(up_k, "dp", n_dp))
            owners.append(row * dp_pair + 1 - dp_col)
    down_flat = jnp.concatenate(down_blocks, axis=0)
    up_flat = jnp.concatenate(up_blocks, axis=0)

    column = jnp.arange(wide, dtype=jnp.int32)
    slot_of = jnp.repeat(jnp.stack(owners), owned * rank) * owned + (column // rank) % owned
    tenant_id = jnp.arange(tenants, dtype=jnp.int32)
    counts = tenant_token_count[0]
    ends = jnp.sum(jnp.where(tenant_id[None, :] <= tenant_id[:, None], counts[None, :], 0), axis=1)
    match = tenant_storage_slot[:, None] == slot_of[None, :]
    end_of = jnp.sum(jnp.where(match, ends[:, None], 0), axis=0)
    start_of = jnp.sum(jnp.where(match, (ends - counts)[:, None], 0), axis=0)
    token = jnp.arange(tok_rows, dtype=jnp.int32)[:, None]
    mask = (start_of[None, :] <= token) & (token < end_of[None, :])
    pick = (column[:, None] % rank == jnp.arange(rank, dtype=jnp.int32)[None, :]).astype(bf16)

    nt = (((1,), (1,)), ((), ()))
    tn = (((0,), (0,)), ((), ()))

    def narrow(rows, table):
        every = lax.dot_general(rows, table, nt, preferred_element_type=f32)
        kept = jnp.where(mask, every, 0.0).astype(bf16)
        return jnp.dot(kept, pick, preferred_element_type=f32)

    def spread(value):
        every = lax.dot_general(value.astype(bf16), pick, nt, preferred_element_type=f32)
        return jnp.where(mask, every, 0.0).astype(bf16)

    partial_sum = jnp.dot(attention_output, frozen_weight, preferred_element_type=f32).astype(bf16)

    def piece(row, col):
        return lax.dynamic_slice_in_dim(partial_sum, (row * t_pair + col) * width, width, 1)

    totals = []
    for k in range(t_rest):
        row = (t_row + k) % t_rest
        total = piece(row, t_col).astype(f32)
        if t_pair == 2:
            total = total + flip(piece(row, 1 - t_col), "tensor", n_tensor).astype(f32)
        totals.append(total.astype(bf16) if k else total)

    both = jnp.concatenate([narrow(attention_output, down_flat), narrow(output_gradient, up_flat)], axis=1)
    *outgoing, both = lax.optimization_barrier((*totals[1:], both))
    base = totals[0]
    for k, total in enumerate(outgoing, 1):
        base = base + shift(total, "tensor", n_tensor, k).astype(f32)
    both = sum_over(both, "tensor", n_tensor)
    low_wide, back_wide = spread(both[:, :rank]), spread(both[:, rank:])

    part_down = 2.0 * lax.dot_general(back_wide, attention_output, tn, preferred_element_type=f32)
    part_up = 2.0 * lax.dot_general(low_wide, output_gradient, tn, preferred_element_type=f32)

    def to_owners(part):
        part = part.astype(bf16).reshape(dp_rest, dp_pair, owned * rank, width)
        grad = None
        for k in [*range(1, dp_rest), 0]:
            total = part[k, 0].astype(f32)
            if dp_pair == 2:
                total = total + flip(part[k, 1], "dp", n_dp).astype(f32)
            if k:
                total = shift(total.astype(bf16), "dp", n_dp, -k).astype(f32)
            grad = total if grad is None else grad + total
        return grad.reshape(owned, rank, width)

    down_gradient = jnp.transpose(to_owners(part_down), (0, 2, 1))
    up_gradient = to_owners(part_up)

    gathered = jnp.zeros((tok_rows, n_tensor * width), bf16)
    for index, block in blocks:
        gathered = lax.dynamic_update_slice_in_dim(gathered, block, index * width, 1)
    grad_base = lax.dot_general(gathered, frozen_weight, nt, preferred_element_type=f32)
    grad_low = jnp.dot(back_wide, down_flat, preferred_element_type=f32)
    input_grad = (grad_base + 2.0 * grad_low).astype(bf16)
    lifted = jnp.dot(low_wide, up_flat, preferred_element_type=f32)
    proj_out = (base + 2.0 * lifted).astype(bf16)

    updated_down_weight, updated_down_first_moment, updated_down_second_moment = adam_update(
        adapter_down_weight, down_first_moment, down_second_moment, down_gradient
    )
    updated_up_weight, updated_up_first_moment, updated_up_second_moment = adam_update(
        adapter_up_weight, up_first_moment, up_second_moment, up_gradient
    )
    return (
        proj_out,
        input_grad,
        updated_down_weight,
        updated_up_weight,
        updated_down_first_moment,
        updated_down_second_moment,
        updated_up_first_moment,
        updated_up_second_moment,
    )


def solution(mesh):
    placed = (
        P("dp", "tensor"),
        P("tensor", None),
        P("dp", "tensor"),
        P("dp", None),
        P(),
        P("dp", "tensor", None),
        P("dp", None, "tensor"),
        P("dp", "tensor", None),
        P("dp", "tensor", None),
        P("dp", None, "tensor"),
        P("dp", None, "tensor"),
    )
    return jax.shard_map(
        functools.partial(local, mesh.shape["dp"], mesh.shape["tensor"]),
        mesh=mesh,
        in_specs=placed,
        out_specs=(
            P("dp", "tensor"),
            P("dp", "tensor"),
            P("dp", "tensor", None),
            P("dp", None, "tensor"),
            P("dp", "tensor", None),
            P("dp", "tensor", None),
            P("dp", None, "tensor"),
            P("dp", None, "tensor"),
        ),
        check_vma=False,
    )
```
